32 devices in a mesh: dp: 2 (over x), crop: 4 (over y, core), tensor: 4 (over z).
Axes of the slice: x: 2, y: 2, z: 4, core: 2. Of those that a mesh axis runs over, the one named last changes fastest.
Arguments:
- hidden_a: bfloat16 [512, 8192], P('crop', 'dp'), as said below
- hidden_b: bfloat16 [512, 8192], P('crop', 'dp'), as said below
- weight: bfloat16 [8192, 8192], P('dp', 'tensor')
Outputs:
- weight_grad: float32 [8192, 8192], P(('dp', 'crop'), 'tensor')
Inputs may be any that keep to these rules, and one draw needn't show every extreme that they name: `hidden_a`: nonnegative entries. `hidden_b`: nonnegative entries.
All inputs are finite; a program needn't handle non-finite values.
Results may differ from the reference program's by a relative error of at most 0.0015.
Values may be sent and summed in bfloat16 or wider, within the bound.
A program may use at most 128 MiB of HBM per device.

```python
import jax
import jax.numpy as jnp
from jax import lax

H = 8192
F = 8192
B = 512


def rising_scale(low, high, count):
    position = jnp.arange(count, dtype=jnp.float32) / jnp.float32(max(count - 1, 1))
    level = jnp.exp(jnp.log(jnp.float32(low)) + position * (jnp.log(jnp.float32(high)) - jnp.log(jnp.float32(low))))
    return level / jnp.sqrt(jnp.mean(level * level))


def hidden_pair(key):
    shared = jnp.clip(jax.random.normal(jax.random.fold_in(key, 21), (B, H), jnp.float32), -6.0, 6.0)
    left_noise = jnp.clip(jax.random.normal(jax.random.fold_in(key, 22), (B, H), jnp.float32), -6.0, 6.0)
    right_noise = jnp.clip(jax.random.normal(jax.random.fold_in(key, 23), (B, H), jnp.float32), -6.0, 6.0)
    row_scale = rising_scale(0.5, 2.5, B)[:, None]
    left = jnp.maximum(shared + 0.6 * left_noise, 0.0) * row_scale
    right = jnp.maximum(shared + 0.6 * right_noise, 0.0) * row_scale
    return (left, right)


def draw_hidden_a(key, part):
    return hidden_pair(key)[0].astype(jnp.bfloat16)


def draw_hidden_b(key, part):
    return hidden_pair(key)[1].astype(jnp.bfloat16)


def draw_weight(key, part):
    base_key = jax.random.fold_in(key, 11)
    band_key = jax.random.fold_in(key, 12)
    level_key = jax.random.fold_in(key, 13)
    base = jnp.clip(jax.random.normal(base_key, (H, F), jnp.float32), -6.0, 6.0) / jnp.sqrt(jnp.float32(H))
    upper = jax.random.bernoulli(band_key, 0.5, (F,))
    level = jax.random.uniform(level_key, (F,), jnp.float32)
    low_scale = jnp.exp(jnp.log(0.4) + level * (jnp.log(0.9) - jnp.log(0.4)))
    high_scale = jnp.exp(jnp.log(2.4) + level * (jnp.log(3.6) - jnp.log(2.4)))
    column_scale = jnp.where(upper, high_scale, low_scale)
    return (base * column_scale[None, :]).astype(jnp.bfloat16)


def setup_inputs(seed: int = 0) -> dict:
    key_of = jax.random.split(jax.random.key(seed), 4)
    hidden_a = draw_hidden_a(jax.random.fold_in(key_of[3], 71), 0)
    hidden_b = draw_hidden_b(jax.random.fold_in(key_of[3], 71), 0)
    weight = draw_weight(jax.random.fold_in(key_of[3], 71), 0)
    return dict(hidden_a=hidden_a, hidden_b=hidden_b, weight=weight)


epsilon = 0.0001

def reference(hidden_a, hidden_b, weight):
    total_rows = hidden_a.shape[0]
    left_proj = jnp.dot(hidden_a, weight, preferred_element_type=jnp.float32).astype(jnp.bfloat16)
    right_proj = jnp.dot(hidden_b, weight, preferred_element_type=jnp.float32).astype(jnp.bfloat16)
    stacked = jnp.stack([left_proj, right_proj]).astype(jnp.float32)
    col_means = lax.optimization_barrier(jnp.mean(stacked, axis=1))
    centered = stacked - col_means[:, None, :]
    spread = lax.optimization_barrier(jnp.sum(centered * centered, axis=1))
    deviation = jnp.sqrt(spread / (total_rows - 1.0) + epsilon)
    rounded = centered.astype(jnp.bfloat16)
    products = []
    for branch in range(2):
        gram_full = lax.dot_general(rounded[branch], rounded[branch], (((1,), (1,)), ((), ())), preferred_element_type=jnp.float32)
        products.append(jnp.dot(gram_full.astype(jnp.bfloat16), rounded[branch], preferred_element_type=jnp.float32))
    products = jnp.stack(products)
    hinge_rate = jnp.where(deviation < 1.0, 25.0 / ((total_rows - 1.0) * deviation), 0.0)[:, None, :]
    differ = stacked[0] - stacked[1]
    pull_term = jnp.stack([differ, -differ]) * (50.0 / total_rows)
    cov_scale = 4.0 / (total_rows - 1.0) ** 2
    row_grads = pull_term - hinge_rate * centered + cov_scale * (products - centered * spread[:, None, :])
    row_grads = row_grads.astype(jnp.bfloat16)
    across = (((0,), (0,)), ((), ()))
    left_term = lax.dot_general(hidden_a, row_grads[0], across, preferred_element_type=jnp.float32)
    right_term = lax.dot_general(hidden_b, row_grads[1], across, preferred_element_type=jnp.float32)
    return left_term + right_term
```

```python
import jax
import jax.numpy as jnp
from jax import lax
from jax.sharding import PartitionSpec as P

epsilon = 0.0001
f32 = jnp.float32
bf16 = jnp.bfloat16


def gather_features(hidden, weight):
    left = jnp.dot(hidden[0], weight, preferred_element_type=f32)
    right = jnp.dot(hidden[1], weight, preferred_element_type=f32)
    mine = lax.psum_scatter(
        jnp.stack([left, right], axis=1), "dp", scatter_dimension=0, tiled=True
    ).astype(bf16)
    whole = lax.all_gather(mine, ("crop", "dp"), axis=0, tiled=True)
    return jnp.stack([whole[:, 0, :], whole[:, 1, :]])


def share_gram(rounded):
    groups = lax.axis_size("dp") * lax.axis_size("crop")
    rows = rounded.shape[1] // groups
    place = lax.axis_index("crop") * lax.axis_size("dp") + lax.axis_index("dp")
    own = lax.dynamic_slice_in_dim(rounded, place * rows, rows, axis=1)
    gram = jnp.einsum("vrf,vbf->vrb", own, rounded, preferred_element_type=f32)
    gram = lax.psum(gram, "tensor").astype(bf16)
    return lax.all_gather(gram, ("crop", "dp"), axis=1, tiled=True)


def body(hidden_a, hidden_b, weight):
    hidden = jnp.stack([hidden_a, hidden_b])
    columns = lax.all_to_all(hidden, "crop", split_axis=2, concat_axis=1, tiled=True)
    low = gather_features((hidden_a, hidden_b), weight)
    stacked = low.astype(f32)
    total_rows = stacked.shape[1]
    col_means = jnp.mean(stacked, axis=1)
    centered = stacked - col_means[:, None, :]
    spread = jnp.sum(centered * centered, axis=1)
    deviation = jnp.sqrt(spread / (total_rows - 1.0) + epsilon)
    rounded = centered.astype(bf16)
    gram_low = share_gram(rounded)
    products = jnp.einsum("vrb,vbf->vrf", gram_low, rounded, preferred_element_type=f32)
    hinge_rate = jnp.where(deviation < 1.0, 25.0 / ((total_rows - 1.0) * deviation), 0.0)[
        :, None, :
    ]
    differ = stacked[0] - stacked[1]
    pull_term = jnp.stack([differ, -differ]) * (50.0 / total_rows)
    cov_scale = 4.0 / (total_rows - 1.0) ** 2
    row_grads = (
        pull_term - hinge_rate * centered + cov_scale * (products - centered * spread[:, None, :])
    ).astype(bf16)
    both = columns.reshape(2 * total_rows, -1)
    grads = row_grads.reshape(2 * total_rows, -1)
    across = (((0,), (0,)), ((), ()))
    return lax.dot_general(both, grads, across, preferred_element_type=f32)


def solution(mesh):
    placed = (P("crop", "dp"), P("crop", "dp"), P("dp", "tensor"))
    return jax.shard_map(
        body, mesh=mesh, in_specs=placed, out_specs=P(("dp", "crop"), "tensor"), check_vma=False
    )
```

```python
import jax
import jax.numpy as jnp
from jax import lax
from jax.sharding import PartitionSpec as P

epsilon = 0.0001
f32 = jnp.float32
bf16 = jnp.bfloat16


def project(hidden, weight):
    both = jnp.concatenate(hidden, axis=0)
    part = jnp.dot(both, weight, preferred_element_type=f32)
    return lax.psum_scatter(part, "dp", scatter_dimension=0, tiled=True).astype(bf16)


def gather_features(mine, view_rows):
    rows, features = mine.shape
    crops = lax.axis_size("crop")
    pieces = view_rows // rows
    whole = lax.all_gather(mine, ("dp", "crop"), axis=0, tiled=True)
    ordered = whole.reshape(2, pieces, crops, rows, features).transpose(0, 2, 1, 3, 4)
    return ordered.reshape(2, crops * view_rows, features)


def share_gram(rounded):
    _, total, features = rounded.shape
    crops = lax.axis_size("crop")
    groups = lax.axis_size("dp") * crops
    rows = 2 * total // groups
    place = lax.axis_index("dp") * crops + lax.axis_index("crop")
    own = lax.dynamic_slice_in_dim(rounded.reshape(2 * total, features), place * rows, rows)
    view = lax.dynamic_index_in_dim(rounded, place * rows // total, keepdims=False)
    gram = lax.dot_general(own, view, (((1,), (1,)), ((), ())), preferred_element_type=f32)
    gram = lax.psum(gram, "tensor").astype(bf16)
    return lax.all_gather(gram, ("dp", "crop"), axis=0, tiled=True).reshape(2, total, total)


def body(hidden_a, hidden_b, weight):
    hidden = jnp.stack([hidden_a, hidden_b])
    columns = lax.all_to_all(hidden, "crop", split_axis=2, concat_axis=1, tiled=True)
    mine = project((hidden_a, hidden_b), weight)
    mine, columns = lax.optimization_barrier((mine, columns))
    low = gather_features(mine, hidden_a.shape[0])
    stacked = low.astype(f32)
    total_rows = stacked.shape[1]
    col_means = jnp.mean(stacked, axis=1)
    centered = stacked - col_means[:, None, :]
    spread = jnp.sum(centered * centered, axis=1)
    deviation = jnp.sqrt(spread / (total_rows - 1.0) + epsilon)
    rounded = centered.astype(bf16)
    gram_low = share_gram(rounded)
    products = jnp.einsum("vrb,vbf->vrf", gram_low, rounded, preferred_element_type=f32)
    hinge_rate = jnp.where(deviation < 1.0, 25.0 / ((total_rows - 1.0) * deviation), 0.0)[
        :, None, :
    ]
    differ = stacked[0] - stacked[1]
    pull_term = jnp.stack([differ, -differ]) * (50.0 / total_rows)
    cov_scale = 4.0 / (total_rows - 1.0) ** 2
    row_grads = (
        pull_term - hinge_rate * centered + cov_scale * (products - centered * spread[:, None, :])
    ).astype(bf16)
    both = columns.reshape(2 * total_rows, -1)
    grads = row_grads.reshape(2 * total_rows, -1)
    across = (((0,), (0,)), ((), ()))
    return lax.dot_general(both, grads, across, preferred_element_type=f32)


def solution(mesh):
    placed = (P("crop", "dp"), P("crop", "dp"), P("dp", "tensor"))
    return jax.shard_map(
        body, mesh=mesh, in_specs=placed, out_specs=P(("dp", "crop"), "tensor"), check_vma=False
    )
```

```python
import jax
import jax.numpy as jnp
from jax import lax
from jax.sharding import PartitionSpec as P

epsilon = 0.0001
f32 = jnp.float32
bf16 = jnp.bfloat16


def project(hidden, weight):
    both = jnp.concatenate(hidden, axis=0)
    part = jnp.dot(both, weight, preferred_element_type=f32)
    return lax.psum_scatter(part, "dp", scatter_dimension=0, tiled=True).astype(bf16)


def gather_features(mine, view_rows):
    rows, features = mine.shape
    crops = lax.axis_size("crop")
    pieces = view_rows // rows
    whole = lax.all_gather(mine, ("dp", "crop"), axis=0, tiled=True)
    ordered = whole.reshape(2, pieces, crops, rows, features).transpose(0, 2, 1, 3, 4)
    return ordered.reshape(2, crops * view_rows, features)


def share_gram(rounded):
    _, total, features = rounded.shape
    crops = lax.axis_size("crop")
    groups = lax.axis_size("dp") * crops
    rows = 2 * total // groups
    place = lax.axis_index("dp") * crops + lax.axis_index("crop")
    own = lax.dynamic_slice_in_dim(rounded.reshape(2 * total, features), place * rows, rows)
    view = lax.dynamic_index_in_dim(rounded, place * rows // total, keepdims=False)
    gram = lax.dot_general(own, view, (((1,), (1,)), ((), ())), preferred_element_type=f32)
    shares = lax.axis_size("tensor")
    slabs = lax.all_to_all(gram, "tensor", split_axis=0, concat_axis=0, tiled=True)
    summed = jnp.sum(slabs.reshape(shares, rows // shares, total), axis=0).astype(bf16)
    whole = lax.all_gather(summed, ("dp", "crop", "tensor"), axis=0, tiled=True)
    return whole.reshape(2, total, total)


def body(hidden_a, hidden_b, weight):
    hidden = jnp.stack([hidden_a, hidden_b])
    columns = lax.all_to_all(hidden, "crop", split_axis=2, concat_axis=1, tiled=True)
    mine = project((hidden_a, hidden_b), weight)
    mine, columns = lax.optimization_barrier((mine, columns))
    low = gather_features(mine, hidden_a.shape[0])
    stacked = low.astype(f32)
    total_rows = stacked.shape[1]
    col_means = jnp.mean(stacked, axis=1)
    centered = stacked - col_means[:, None, :]
    spread = jnp.sum(centered * centered, axis=1)
    deviation = jnp.sqrt(spread / (total_rows - 1.0) + epsilon)
    rounded = centered.astype(bf16)
    gram_low = share_gram(rounded)
    products = jnp.einsum("vrb,vbf->vrf", gram_low, rounded, preferred_element_type=f32)
    hinge_rate = jnp.where(deviation < 1.0, 25.0 / ((total_rows - 1.0) * deviation), 0.0)[
        :, None, :
    ]
    differ = stacked[0] - stacked[1]
    pull_term = jnp.stack([differ, -differ]) * (50.0 / total_rows)
    cov_scale = 4.0 / (total_rows - 1.0) ** 2
    row_grads = (
        pull_term - hinge_rate * centered + cov_scale * (products - centered * spread[:, None, :])
    ).astype(bf16)
    both = columns.reshape(2 * total_rows, -1)
    grads = row_grads.reshape(2 * total_rows, -1)
    across = (((0,), (0,)), ((), ()))
    return lax.dot_general(both, grads, across, preferred_element_type=f32)


def solution(mesh):
    placed = (P("crop", "dp"), P("crop", "dp"), P("dp", "tensor"))
    return jax.shard_map(
        body, mesh=mesh, in_specs=placed, out_specs=P(("dp", "crop"), "tensor"), check_vma=False
    )
```
